1024 devices in a mesh: gz: 16 (over x, y), gy: 64 (over z, core).
Axes of the slice: x: 4, y: 4, z: 32, core: 2. Of those that a mesh axis runs over, the one named last changes fastest.
Arguments:
- grid_grad: float32 [256, 1024, 512], P('gz', 'gy'), may hold values from -6 to 6
- cells: int32 [3, 2097152], P(None, ('gz', 'gy')), may hold values from 0 to 1023, as said below
- offsets: int32 [3, 2097152], P(None, ('gz', 'gy')), may hold values from 0 to 1023
- owners: int32 [2097152, 1], P(('gz', 'gy')), may hold values from 0 to 1023; in each aligned block of 2048 rows (0 to 2047, 2048 to 4095, ...) at most 4 rows name the same one
- slots: int32 [2097152], P(('gz', 'gy')), may hold values from 0 to 2047
Outputs:
- pos_grad: float32 [3, 2097152], P(None, ('gz', 'gy'))
The draws below stay inside these ranges and needn't reach their ends.
Inputs may be any that keep to these rules, and one draw needn't show every extreme that they name: `cells`: the row's cell lies in the mesh block of the device that holds the row: along z in [gz * 16, gz * 16 + 16), along y in [gy * 16, gy * 16 + 16), where gz, gy are that device's indices. `owners`: owners are linear device indices gz * 64 + gy. Among the rows of one device, no owner is named by more than 4 rows; some owner is named by exactly 4.
All inputs are finite; a program needn't handle non-finite values.
Results may differ from the reference program's by a relative error of at most 0.0003.
Values sent between devices are 32-bit elements; how exact they have to be, the bound alone decides.
No kernel may reach another device: no remote copies, remote signals or barrier semaphores. Data moves between devices by JAX's collectives and lax.ppermute only.
A program may use at most 32 MiB of HBM per device.

```python
import math
import jax
import jax.numpy as jnp
import numpy as np

CZ = 16
CY = 16
LX = 512
P_DEV = 2048
NZ = 256
NY = 1024
PROWS = 2097152
CAP = 4
N_GZ = 16
N_GY = 64
DEVICES = 1024


def draw_cells(key, part):
    total_rows = P_DEV * N_GZ * N_GY
    device = jnp.arange(total_rows, dtype=jnp.int32) // P_DEV
    index_z = device // N_GY
    index_y = device % N_GY
    key_z = jax.random.fold_in(key, 11)
    key_y = jax.random.fold_in(key, 12)
    key_x = jax.random.fold_in(key, 13)
    cell_z = index_z * CZ + jax.random.randint(key_z, (total_rows,), 0, CZ, dtype=jnp.int32)
    cell_y = index_y * CY + jax.random.randint(key_y, (total_rows,), 0, CY, dtype=jnp.int32)
    cell_x = jax.random.randint(key_x, (total_rows,), 0, LX, dtype=jnp.int32)
    return jnp.stack([cell_z, cell_y, cell_x]).astype(jnp.int32)


def set_ends(result, rng, low, largest):
    extent = result.shape
    place = [jax.random.randint(jax.random.fold_in(rng, axis), (), 0, extent[axis]) for axis in range(len(extent))]
    result = result.at[tuple(place)].set(low)
    longest = extent.index(max(extent))
    place[longest] = (place[longest] + 1) % extent[longest]
    return result.at[tuple(place)].set(largest)


def levels(stream_key, shape, pieces, smallest, largest):
    def one(dim, shards_of):
        heights = jax.random.uniform(jax.random.fold_in(jax.random.fold_in(stream_key, 6), dim), (shards_of,), jnp.float32, smallest / len(pieces), largest / len(pieces))
        return jnp.repeat(jnp.exp(heights), shape[dim] // shards_of).reshape((-1,) + (1,) * (len(shape) - dim - 1))

    gain = one(*pieces[0])
    for cut in pieces[1:]:
        gain = gain * one(*cut)
    return gain


def shared_out(rng, own, number, rows, count, top, bound, lean):
    ranking = jax.random.permutation(rng, count)
    heavy_load, ordinary = load_shares(count, rows * top, bound, lean, True), load_shares(count, rows * top, bound, lean, False)
    places = jnp.arange(count)

    def named(sizes, rotation):
        used = int((sizes > 0).sum())
        fixed = max(1, used // 4)
        passed = fixed + (places - fixed + rotation * (used - fixed)) % max(1, count - fixed)
        return jnp.zeros((count,), jnp.int32).at[ranking[jnp.where(places < fixed, places, passed)]].set(jnp.asarray(sizes, jnp.int32))

    sizes = jnp.where(number % 4 == 0, named(heavy_load, number // 4), named(ordinary, number - number // 4 - 1))
    mixed = jax.random.permutation(jax.random.fold_in(own, 3), count)
    source_of, sink = mixed[0:count // 2 * 2:2], mixed[1:count // 2 * 2:2]
    room = jnp.minimum(sizes[source_of] - 1, bound - sizes[sink]) // 2
    room = jnp.where((source_of == ranking[0]) | (sink == ranking[0]) | (sizes[sink] == 0), 0, jnp.maximum(room, 0))
    passed = jax.random.randint(jax.random.fold_in(own, 4), (count // 2,), 0, 1 << 20) % (room + 1)
    sizes = sizes.at[source_of].add(-passed).at[sink].add(passed)
    members = jnp.searchsorted(jnp.cumsum(sizes), jnp.arange(rows * top), side="right").astype(jnp.int32)
    table = members.reshape(top, rows).T
    table = table[jax.random.permutation(jax.random.fold_in(own, 1), rows)]
    rotation = jax.random.randint(jax.random.fold_in(own, 2), (rows, 1), 0, top)
    return jnp.take_along_axis(table, (jnp.arange(top)[None, :] + rotation) % top, axis=1)


def load_shares(number_of, total, most, skew, full):
    loads = [(1 << 20) // math.isqrt(standing ** skew) + 1 for standing in range(1, number_of + 1)]
    largest = most if full else min(most, max(-(-total // number_of), total * loads[0] // sum(loads)))
    least = 1 if total - largest >= number_of - 1 else 0
    holding, surplus = [largest] + [least] * (number_of - 1), total - largest - least * (number_of - 1)
    while surplus > 0:
        free = [i for i in range(1, number_of) if holding[i] < largest] or [i for i in range(1, number_of) if holding[i] < most]
        pool, remaining = sum([loads[i] for i in free]), surplus
        for i in free:
            extra = min(most - holding[i], max(1, remaining * loads[i] // pool), surplus)
            holding[i] = holding[i] + extra
            surplus = surplus - extra
    return np.array(holding)


def scatter_about(stream_key, extent, spread, limit, pieces=(), kind=jnp.bfloat16):
    loudness = levels(stream_key, extent, pieces, -0.22, 0.18) if pieces else 1.0
    array = jax.random.normal(stream_key, extent, jnp.float32) * spread * loudness
    return jnp.minimum(jnp.maximum(array, -limit), limit).astype(kind)


def setup_inputs(seed: int = 0) -> dict:
    streams_of = jax.random.split(jax.random.key(seed), 6)
    grid_grad = scatter_about(streams_of[0], (NZ, NY, LX), 1.0, 6.0, ((0, 16), (1, 64)), jnp.float32)
    cells = draw_cells(jax.random.fold_in(streams_of[5], 71), 0)
    offsets = set_ends(jax.random.randint(streams_of[2], (3, PROWS), 0, 1024), jax.random.fold_in(streams_of[2], 1), 0, 1023).astype(jnp.int32)
    owners_keys = jax.random.split(jax.random.fold_in(streams_of[3], 1), PROWS // P_DEV)
    owners_turns = jax.random.permutation(jax.random.fold_in(streams_of[3], 3), PROWS // P_DEV)
    owners = jax.vmap(lambda own, number: shared_out(jax.random.fold_in(streams_of[3], 2), own, number, P_DEV, DEVICES, 1, CAP, 2))(owners_keys, owners_turns).reshape((PROWS, 1))
    slots = set_ends(jax.random.randint(streams_of[4], (PROWS,), 0, P_DEV), jax.random.fold_in(streams_of[4], 1), 0, P_DEV - 1).astype(jnp.int32)
    return {"grid_grad": grid_grad, "cells": cells, "offsets": offsets, "owners": owners, "slots": slots}


def cic_gradient(corner, fraction):
    weight_z = (1.0 - fraction[0], fraction[0])
    weight_y = (1.0 - fraction[1], fraction[1])
    weight_x = (1.0 - fraction[2], fraction[2])
    grad_z = jnp.zeros_like(fraction[0])
    grad_y = jnp.zeros_like(fraction[0])
    grad_x = jnp.zeros_like(fraction[0])
    for first in range(2):
        for second in range(2):
            grad_z = grad_z + (corner[1][first][second] - corner[0][first][second]) * weight_y[first] * weight_x[second]
            grad_y = grad_y + (corner[first][1][second] - corner[first][0][second]) * weight_z[first] * weight_x[second]
            grad_x = grad_x + (corner[first][second][1] - corner[first][second][0]) * weight_z[first] * weight_y[second]
    return jnp.stack([grad_z, grad_y, grad_x])


def reference(grid_grad, cells, offsets, owners, slots):
    size_z, size_y, size_x = grid_grad.shape
    fraction = (offsets.astype(jnp.float32) + 0.5) / 1024.0
    flat = grid_grad.reshape(-1)
    corner = []
    for step_z in range(2):
        plane = []
        for step_y in range(2):
            line = []
            for step_x in range(2):
                pos_z = (cells[0] + step_z) % size_z
                pos_y = (cells[1] + step_y) % size_y
                pos_x = (cells[2] + step_x) % size_x
                line.append(flat[(pos_z * size_y + pos_y) * size_x + pos_x])
            plane.append(line)
        corner.append(plane)
    gradient = cic_gradient(corner, fraction)
    target = (owners[:, 0] * P_DEV + slots).astype(jnp.int32)
    total = jnp.zeros((3, cells.shape[1]), jnp.float32)
    return total.at[:, target].add(gradient)
```

```python
import jax
import jax.numpy as jnp
from jax import lax
from jax.experimental import pallas as pl
from jax.experimental.pallas import tpu as pltpu
from jax.sharding import Mesh, PartitionSpec as P

F32 = jnp.float32
BF16 = jnp.bfloat16
TILE = 256


def split(x):
    high = x.astype(BF16)
    return high, (x - high.astype(F32)).astype(BF16)


def hot(mask):
    return jnp.where(mask, 1.0, 0.0).astype(BF16)


def rows_of(shape):
    return lax.broadcasted_iota(jnp.int32, shape, 0)


def lane_tile(ref, row, t):
    return ref[row : row + 1, t * TILE : (t + 1) * TILE]


def fraction_of(offsets):
    return (offsets.astype(F32) + 0.5) / 1024.0


def two_weights(index, frac, place):
    lower = place == index
    upper = place == index + 1
    weight = jnp.where(lower, 1.0 - frac, jnp.where(upper, frac, 0.0))
    slope = jnp.where(upper, 1.0, jnp.where(lower, -1.0, 0.0))
    return weight, slope


def with_next_x(block):
    return block, pltpu.roll(block, block.shape[1] - 1, 1) - block


def count_earlier(owner_row):
    num_rows = owner_row.shape[1]
    chunks = num_rows // 128
    names = owner_row.astype(F32)
    columns = jnp.concatenate([names[:, i * 128 : (i + 1) * 128] for i in range(chunks)], 0)
    columns = jnp.concatenate([columns, jnp.zeros((128 - chunks, 128), F32)], 0).T
    earlier = rows_of((128, 128)) < lax.broadcasted_iota(jnp.int32, (128, 128), 1)
    counts = [jnp.zeros((8, 128), F32)] * chunks
    for i in range(chunks):
        column = jnp.broadcast_to(columns[:, i : i + 1], (128, 128))
        for j in range(i, chunks):
            same = column == names[:, j * 128 : (j + 1) * 128]
            if i == j:
                same = same & earlier
            ones = jnp.where(same, 1.0, 0.0)
            counts[j] = counts[j] + jnp.sum(ones.reshape(16, 8, 128), axis=0)
    return jnp.concatenate([jnp.sum(c, axis=0, keepdims=True) for c in counts], 1)


def inner_kernel(grid_ref, cells_ref, offsets_ref, owners_ref, grad_ref, place_ref, lhs_ref):
    rows, size_x = grid_ref.shape
    for part, block in enumerate(with_next_x(grid_ref[...])):
        for half, piece in enumerate(split(block)):
            lhs_ref[part * rows : (part + 1) * rows, half * size_x : (half + 1) * size_x] = piece
    owners = owners_ref[...]
    rank = count_earlier(owners).astype(jnp.int32)
    place_ref[...] = ((owners >> 6) * 2 + (owners & 1)) * 4 + rank
    for t in range(cells_ref.shape[1] // TILE):
        at_x = hot(rows_of((size_x, TILE)) == lane_tile(cells_ref, 2, t))
        read = jnp.dot(lhs_ref[...], jnp.concatenate([at_x, at_x], 0), preferred_element_type=F32)
        frac = [fraction_of(lane_tile(offsets_ref, a, t)) for a in range(3)]
        index_z = lane_tile(cells_ref, 0, t) & 15
        index_y = lane_tile(cells_ref, 1, t) & 15
        sum_z = sum_y = sum_x = jnp.zeros((16, TILE), F32)
        for z in range(16):
            diff = read[rows + z * 16 : rows + (z + 1) * 16]
            value = read[z * 16 : (z + 1) * 16] + diff * frac[2]
            weight_z, slope_z = two_weights(index_z, frac[0], z)
            sum_z = sum_z + value * slope_z
            sum_y = sum_y + value * weight_z
            sum_x = sum_x + diff * weight_z
        weight_y, slope_y = two_weights(index_y, frac[1], rows_of((16, TILE)))
        parts = [sum_z * weight_y, sum_y * slope_y, sum_x * weight_y]
        sums = [jnp.sum(p, axis=0, keepdims=True) for p in parts]
        grad_ref[:, t * TILE : (t + 1) * TILE] = jnp.concatenate(
            sums + [jnp.zeros((5, TILE), F32)], 0
        )


def send_kernel(
    face_z_ref, face_y_ref, edge_ref, grad_ref, place_ref, cells_ref, offsets_ref, owners_ref,
    slots_ref, send_ref, halo_ref, value_ref, hot_ref,
):
    size_x = edge_ref.shape[1]
    edge = jnp.broadcast_to(edge_ref[...], (8, size_x))
    halo = jnp.concatenate([face_z_ref[...], face_y_ref[...], edge], 0)
    count = halo.shape[0]
    for part, block in enumerate(with_next_x(halo)):
        for half, piece in enumerate(split(block)):
            halo_ref[(2 * half + part) * count : (2 * half + part + 1) * count, :] = piece
    for t in range(cells_ref.shape[1] // TILE):
        lanes = slice(t * TILE, (t + 1) * TILE)
        at_x = hot(rows_of((size_x, TILE)) == lane_tile(cells_ref, 2, t))
        read = jnp.dot(halo_ref[...], at_x, preferred_element_type=F32)
        read = read[: 2 * count] + read[2 * count :]
        frac = [fraction_of(lane_tile(offsets_ref, a, t)) for a in range(3)]
        index_z = lane_tile(cells_ref, 0, t) & 15
        index_y = lane_tile(cells_ref, 1, t) & 15
        diff = read[count:]
        value = read[:count] + diff * frac[2]
        weight_z, slope_z = two_weights(index_z, frac[0], rows_of((16, TILE)))
        weight_y, slope_y = two_weights(index_y, frac[1], rows_of((16, TILE)))
        top_z, step_z = two_weights(index_z, frac[0], 16)
        top_y, step_y = two_weights(index_y, frac[1], 16)

        def over(block, weight):
            return jnp.sum(block * weight, axis=0, keepdims=True)

        on_z, on_y, on_edge = value[:16], value[16:32], value[32:33]
        dif_z, dif_y, dif_edge = diff[:16], diff[16:32], diff[32:33]
        grad_z = step_z * (over(on_z, weight_y) + top_y * on_edge) + top_y * over(on_y, slope_z)
        grad_y = top_z * (over(on_z, slope_y) + step_y * on_edge) + step_y * over(on_y, weight_z)
        grad_x = top_z * (over(dif_z, weight_y) + top_y * dif_edge) + top_y * over(dif_y, weight_z)
        grad_z = grad_z + grad_ref[0:1, lanes]
        grad_y = grad_y + grad_ref[1:2, lanes]
        grad_x = grad_x + grad_ref[2:3, lanes]
        slot = slots_ref[:, lanes].astype(F32)
        kind = rows_of((8, TILE)) & 3
        four = jnp.where(
            kind == 0, grad_z, jnp.where(kind == 1, grad_y, jnp.where(kind == 2, grad_x, slot))
        )
        owner_z = (owners_ref[:, lanes] >> 1) & 31
        here = (rows_of((128, TILE)) >> 2) == owner_z
        for half, piece in enumerate(split(four)):
            tall = jnp.concatenate([piece.astype(F32)] * 16, 0)
            value_ref[half * 128 : (half + 1) * 128, lanes] = jnp.where(here, tall, 0.0).astype(BF16)
        hot_ref[:, lanes] = hot(rows_of((128, TILE)) == place_ref[:, lanes])
    both = lax.dot_general(
        value_ref[...], hot_ref[...], (((1,), (1,)), ((), ())), preferred_element_type=F32
    )
    send_ref[...] = both[:128] + both[128:]


def turn_kernel(in_ref, out_ref):
    out_ref[...] = in_ref[...].T


def place_kernel(recv_ref, out_ref, value_ref, hot_ref):
    turned = recv_ref[...].T
    high, low = split(turned)
    halves = (high.astype(F32), low.astype(F32))
    for j in range(32):
        lanes = slice(j * 128, (j + 1) * 128)
        slot = turned[4 * j + 3 : 4 * j + 4].astype(jnp.int32)
        here = (rows_of((64, 128)) >> 2) == (slot >> 7)
        for half, piece in enumerate(halves):
            four = piece[4 * j : 4 * j + 4]
            eight = jnp.concatenate([four, four], 0)
            tall = jnp.concatenate([eight] * 8, 0)
            value_ref[half * 64 : (half + 1) * 64, lanes] = jnp.where(here, tall, 0.0).astype(BF16)
        hot_ref[:, lanes] = hot(rows_of((128, 128)) == (slot & 127))
    both = lax.dot_general(
        value_ref[...], hot_ref[...], (((1,), (1,)), ((), ())), preferred_element_type=F32
    )
    total = both[:64] + both[64:]
    for h in range(16):
        out_ref[:, h * 128 : (h + 1) * 128] = total[4 * h : 4 * h + 3]


def run_inner(plane, cells, offsets, owner_row):
    rows, size_x = plane.shape
    num_rows = cells.shape[1]
    return pl.pallas_call(
        inner_kernel,
        out_shape=(
            jax.ShapeDtypeStruct((8, num_rows), F32),
            jax.ShapeDtypeStruct((1, num_rows), jnp.int32),
        ),
        scratch_shapes=[pltpu.VMEM((2 * rows, 2 * size_x), BF16)],
        cost_estimate=pl.CostEstimate(
            flops=8 * rows * size_x * num_rows, bytes_accessed=1000000, transcendentals=0
        ),
        name="inner",
    )(plane, cells, offsets, owner_row)


def run_send(face_z, face_y, edge, grad, place, cells, offsets, owner_row, slot_row):
    num_rows = cells.shape[1]
    return pl.pallas_call(
        send_kernel,
        out_shape=jax.ShapeDtypeStruct((128, 128), F32),
        scratch_shapes=[
            pltpu.VMEM((160, edge.shape[1]), BF16),
            pltpu.VMEM((256, num_rows), BF16),
            pltpu.VMEM((128, num_rows), BF16),
        ],
        name="send",
    )(face_z, face_y, edge, grad, place, cells, offsets, owner_row, slot_row)


def run_turn(x):
    return pl.pallas_call(
        turn_kernel, out_shape=jax.ShapeDtypeStruct((128, 128), F32), name="turn"
    )(x)


def run_place(received, num_rows):
    return pl.pallas_call(
        place_kernel,
        out_shape=jax.ShapeDtypeStruct((3, num_rows), F32),
        scratch_shapes=[pltpu.VMEM((128, 4096), BF16), pltpu.VMEM((128, 4096), BF16)],
        name="place",
    )(received)


def body(grid_grad, cells, offsets, owners, slots):
    block_z, block_y, size_x = grid_grad.shape
    num_rows = cells.shape[1]
    count_z = lax.axis_size("gz")
    count_y = lax.axis_size("z") * lax.axis_size("c")
    next_z = [((i + 1) % count_z, i) for i in range(count_z)]
    next_y = [((i + 1) % count_y, i) for i in range(count_y)]
    next_zy = [
        (sz * count_y + sy, dz * count_y + dy) for sz, dz in next_z for sy, dy in next_y
    ]
    face_z = lax.ppermute(grid_grad[0], "gz", next_z)
    face_y = lax.ppermute(grid_grad[:, 0], ("z", "c"), next_y)
    edge = lax.ppermute(grid_grad[0, :1], ("gz", "z", "c"), next_zy)
    owner_row = owners.reshape(1, num_rows)
    slot_row = slots.reshape(1, num_rows)
    plane = grid_grad.reshape(block_z * block_y, size_x)
    grad, place = run_inner(plane, cells, offsets, owner_row)
    send = run_send(face_z, face_y, edge, grad, place, cells, offsets, owner_row, slot_row)
    along_z = lax.all_to_all(send, "z", 0, 0, tiled=True)
    received = lax.all_to_all(run_turn(along_z), ("gz", "c"), 0, 0, tiled=True)
    return run_place(received, num_rows)


def solution(mesh):
    fine = Mesh(mesh.devices.reshape(16, 32, 2), ("gz", "z", "c"))
    every = ("gz", "z", "c")
    placed = (P("gz", ("z", "c"), None), P(None, every), P(None, every), P(every, None), P(every))
    return jax.shard_map(
        body, mesh=fine, in_specs=placed, out_specs=P(None, every), check_vma=False
    )
```

```python
import jax
import jax.numpy as jnp
from jax import lax
from jax.experimental import pallas as pl
from jax.experimental.pallas import tpu as pltpu
from jax.sharding import Mesh, PartitionSpec as P

F32 = jnp.float32
BF16 = jnp.bfloat16
TILE = 256
SMALL = pltpu.CompilerParams(vmem_limit_bytes=16 * 1024 * 1024)


def split(x):
    high = x.astype(BF16)
    return high, (x - high.astype(F32)).astype(BF16)


def hot(mask):
    return jnp.where(mask, 1.0, 0.0).astype(BF16)


def rows_of(shape):
    return lax.broadcasted_iota(jnp.int32, shape, 0)


def lane_tile(ref, row, t):
    return ref[row : row + 1, t * TILE : (t + 1) * TILE]


def fraction_of(offsets):
    return (offsets.astype(F32) + 0.5) / 1024.0


def two_weights(index, frac, place):
    lower = place == index
    upper = place == index + 1
    weight = jnp.where(lower, 1.0 - frac, jnp.where(upper, frac, 0.0))
    slope = jnp.where(upper, 1.0, jnp.where(lower, -1.0, 0.0))
    return weight, slope


def with_next_x(block):
    return block, pltpu.roll(block, block.shape[1] - 1, 1) - block


def count_earlier(owner_row):
    num_rows = owner_row.shape[1]
    chunks = num_rows // 128
    names = owner_row.astype(F32)
    columns = jnp.concatenate([names[:, i * 128 : (i + 1) * 128] for i in range(chunks)], 0)
    columns = jnp.concatenate([columns, jnp.zeros((128 - chunks, 128), F32)], 0).T
    earlier = rows_of((128, 128)) < lax.broadcasted_iota(jnp.int32, (128, 128), 1)
    counts = [jnp.zeros((8, 128), F32)] * chunks
    for i in range(chunks):
        column = jnp.broadcast_to(columns[:, i : i + 1], (128, 128))
        for j in range(i, chunks):
            same = column == names[:, j * 128 : (j + 1) * 128]
            if i == j:
                same = same & earlier
            ones = jnp.where(same, 1.0, 0.0)
            counts[j] = counts[j] + jnp.sum(ones.reshape(16, 8, 128), axis=0)
    return jnp.concatenate([jnp.sum(c, axis=0, keepdims=True) for c in counts], 1)


def faces_kernel(grid_ref, face_z_ref, face_y_ref, edge_ref):
    block_z, block_y = face_y_ref.shape[0], face_z_ref.shape[0]
    face_z_ref[...] = grid_ref[:block_y]
    edge_ref[...] = grid_ref[:1]
    for z in range(block_z):
        face_y_ref[z : z + 1] = grid_ref[z * block_y : z * block_y + 1]


def inner_kernel(grid_ref, cells_ref, offsets_ref, owners_ref, grad_ref, place_ref, lhs_ref):
    rows, size_x = grid_ref.shape
    for part, block in enumerate(with_next_x(grid_ref[...])):
        for half, piece in enumerate(split(block)):
            lhs_ref[part * rows : (part + 1) * rows, half * size_x : (half + 1) * size_x] = piece
    owners = owners_ref[...]
    rank = count_earlier(owners).astype(jnp.int32)
    place_ref[...] = ((owners >> 6) * 2 + (owners & 1)) * 4 + rank
    for t in range(cells_ref.shape[1] // TILE):
        at_x = hot(rows_of((size_x, TILE)) == lane_tile(cells_ref, 2, t))
        read = jnp.dot(lhs_ref[...], jnp.concatenate([at_x, at_x], 0), preferred_element_type=F32)
        frac = [fraction_of(lane_tile(offsets_ref, a, t)) for a in range(3)]
        index_z = lane_tile(cells_ref, 0, t) & 15
        index_y = lane_tile(cells_ref, 1, t) & 15
        sum_z = sum_y = sum_x = jnp.zeros((16, TILE), F32)
        for z in range(16):
            diff = read[rows + z * 16 : rows + (z + 1) * 16]
            value = read[z * 16 : (z + 1) * 16] + diff * frac[2]
            weight_z, slope_z = two_weights(index_z, frac[0], z)
            sum_z = sum_z + value * slope_z
            sum_y = sum_y + value * weight_z
            sum_x = sum_x + diff * weight_z
        weight_y, slope_y = two_weights(index_y, frac[1], rows_of((16, TILE)))
        parts = [sum_z * weight_y, sum_y * slope_y, sum_x * weight_y]
        sums = [jnp.sum(p, axis=0, keepdims=True) for p in parts]
        grad_ref[:, t * TILE : (t + 1) * TILE] = jnp.concatenate(
            sums + [jnp.zeros((5, TILE), F32)], 0
        )


def send_kernel(
    face_z_ref, face_y_ref, edge_ref, grad_ref, place_ref, cells_ref, offsets_ref, owners_ref,
    slots_ref, send_ref, halo_ref, value_ref, hot_ref,
):
    size_x = edge_ref.shape[1]
    edge = jnp.broadcast_to(edge_ref[...], (8, size_x))
    halo = jnp.concatenate([face_z_ref[...], face_y_ref[...], edge], 0)
    count = halo.shape[0]
    for part, block in enumerate(with_next_x(halo)):
        for half, piece in enumerate(split(block)):
            halo_ref[(2 * half + part) * count : (2 * half + part + 1) * count, :] = piece
    for t in range(cells_ref.shape[1] // TILE):
        lanes = slice(t * TILE, (t + 1) * TILE)
        at_x = hot(rows_of((size_x, TILE)) == lane_tile(cells_ref, 2, t))
        read = jnp.dot(halo_ref[...], at_x, preferred_element_type=F32)
        read = read[: 2 * count] + read[2 * count :]
        frac = [fraction_of(lane_tile(offsets_ref, a, t)) for a in range(3)]
        index_z = lane_tile(cells_ref, 0, t) & 15
        index_y = lane_tile(cells_ref, 1, t) & 15
        diff = read[count:]
        value = read[:count] + diff * frac[2]
        weight_z, slope_z = two_weights(index_z, frac[0], rows_of((16, TILE)))
        weight_y, slope_y = two_weights(index_y, frac[1], rows_of((16, TILE)))
        top_z, step_z = two_weights(index_z, frac[0], 16)
        top_y, step_y = two_weights(index_y, frac[1], 16)

        def over(block, weight):
            return jnp.sum(block * weight, axis=0, keepdims=True)

        on_z, on_y, on_edge = value[:16], value[16:32], value[32:33]
        dif_z, dif_y, dif_edge = diff[:16], diff[16:32], diff[32:33]
        grad_z = step_z * (over(on_z, weight_y) + top_y * on_edge) + top_y * over(on_y, slope_z)
        grad_y = top_z * (over(on_z, slope_y) + step_y * on_edge) + step_y * over(on_y, weight_z)
        grad_x = top_z * (over(dif_z, weight_y) + top_y * dif_edge) + top_y * over(dif_y, weight_z)
        grad_z = grad_z + grad_ref[0:1, lanes]
        grad_y = grad_y + grad_ref[1:2, lanes]
        grad_x = grad_x + grad_ref[2:3, lanes]
        slot = slots_ref[:, lanes].astype(F32)
        kind = rows_of((8, TILE)) & 3
        four = jnp.where(
            kind == 0, grad_z, jnp.where(kind == 1, grad_y, jnp.where(kind == 2, grad_x, slot))
        )
        owner_z = (owners_ref[:, lanes] >> 1) & 31
        here = (rows_of((128, TILE)) >> 2) == owner_z
        for half, piece in enumerate(split(four)):
            tall = jnp.concatenate([piece.astype(F32)] * 16, 0)
            value_ref[half * 128 : (half + 1) * 128, lanes] = jnp.where(here, tall, 0.0).astype(BF16)
        hot_ref[:, lanes] = hot(rows_of((128, TILE)) == place_ref[:, lanes])
    both = lax.dot_general(
        value_ref[...], hot_ref[...], (((1,), (1,)), ((), ())), preferred_element_type=F32
    )
    send_ref[...] = both[:128] + both[128:]


def turn_kernel(in_ref, out_ref):
    out_ref[...] = in_ref[...].T


def place_kernel(recv_ref, out_ref, value_ref, hot_ref):
    turned = recv_ref[...].T
    high, low = split(turned)
    halves = (high.astype(F32), low.astype(F32))
    for j in range(32):
        lanes = slice(j * 128, (j + 1) * 128)
        slot = turned[4 * j + 3 : 4 * j + 4].astype(jnp.int32)
        here = (rows_of((64, 128)) >> 2) == (slot >> 7)
        for half, piece in enumerate(halves):
            four = piece[4 * j : 4 * j + 4]
            eight = jnp.concatenate([four, four], 0)
            tall = jnp.concatenate([eight] * 8, 0)
            value_ref[half * 64 : (half + 1) * 64, lanes] = jnp.where(here, tall, 0.0).astype(BF16)
        hot_ref[:, lanes] = hot(rows_of((128, 128)) == (slot & 127))
    both = lax.dot_general(
        value_ref[...], hot_ref[...], (((1,), (1,)), ((), ())), preferred_element_type=F32
    )
    total = both[:64] + both[64:]
    for h in range(16):
        out_ref[:, h * 128 : (h + 1) * 128] = total[4 * h : 4 * h + 3]


def run_faces(plane, block_z, block_y):
    size_x = plane.shape[1]
    return pl.pallas_call(
        faces_kernel,
        out_shape=(
            jax.ShapeDtypeStruct((block_y, size_x), F32),
            jax.ShapeDtypeStruct((block_z, size_x), F32),
            jax.ShapeDtypeStruct((1, size_x), F32),
        ),
        compiler_params=SMALL,
        name="faces",
    )(plane)


def run_inner(plane, cells, offsets, owner_row):
    rows, size_x = plane.shape
    num_rows = cells.shape[1]
    return pl.pallas_call(
        inner_kernel,
        out_shape=(
            jax.ShapeDtypeStruct((8, num_rows), F32),
            jax.ShapeDtypeStruct((1, num_rows), jnp.int32),
        ),
        scratch_shapes=[pltpu.VMEM((2 * rows, 2 * size_x), BF16)],
        compiler_params=SMALL,
        cost_estimate=pl.CostEstimate(
            flops=8 * rows * size_x * num_rows, bytes_accessed=1000000, transcendentals=0
        ),
        name="inner",
    )(plane, cells, offsets, owner_row)


def run_send(face_z, face_y, edge, grad, place, cells, offsets, owner_row, slot_row):
    num_rows = cells.shape[1]
    return pl.pallas_call(
        send_kernel,
        out_shape=jax.ShapeDtypeStruct((128, 128), F32),
        scratch_shapes=[
            pltpu.VMEM((160, edge.shape[1]), BF16),
            pltpu.VMEM((256, num_rows), BF16),
            pltpu.VMEM((128, num_rows), BF16),
        ],
        compiler_params=SMALL,
        name="send",
    )(face_z, face_y, edge, grad, place, cells, offsets, owner_row, slot_row)


def run_turn(x):
    return pl.pallas_call(
        turn_kernel,
        out_shape=jax.ShapeDtypeStruct((128, 128), F32),
        compiler_params=SMALL,
        name="turn",
    )(x)


def run_place(received, num_rows):
    return pl.pallas_call(
        place_kernel,
        out_shape=jax.ShapeDtypeStruct((3, num_rows), F32),
        scratch_shapes=[pltpu.VMEM((128, 4096), BF16), pltpu.VMEM((128, 4096), BF16)],
        compiler_params=SMALL,
        name="place",
    )(received)


def body(grid_grad, cells, offsets, owners, slots):
    block_z, block_y, size_x = grid_grad.shape
    num_rows = cells.shape[1]
    count_z = lax.axis_size("gz")
    count_y = lax.axis_size("z") * lax.axis_size("c")
    next_z = [((i + 1) % count_z, i) for i in range(count_z)]
    next_y = [((i + 1) % count_y, i) for i in range(count_y)]
    next_zy = [
        (sz * count_y + sy, dz * count_y + dy) for sz, dz in next_z for sy, dy in next_y
    ]
    plane = grid_grad.reshape(block_z * block_y, size_x)
    face_z, face_y, edge = run_faces(plane, block_z, block_y)
    face_z = lax.ppermute(face_z, "gz", next_z)
    face_y = lax.ppermute(face_y, ("z", "c"), next_y)
    edge = lax.ppermute(edge, ("gz", "z", "c"), next_zy)
    owner_row = owners.reshape(1, num_rows)
    slot_row = slots.reshape(1, num_rows)
    grad, place = run_inner(plane, cells, offsets, owner_row)
    send = run_send(face_z, face_y, edge, grad, place, cells, offsets, owner_row, slot_row)
    along_z = lax.all_to_all(send, "z", 0, 0, tiled=True)
    received = lax.all_to_all(run_turn(along_z), ("gz", "c"), 0, 0, tiled=True)
    return run_place(received, num_rows)


def solution(mesh):
    fine = Mesh(mesh.devices.reshape(16, 32, 2), ("gz", "z", "c"))
    every = ("gz", "z", "c")
    placed = (P("gz", ("z", "c"), None), P(None, every), P(None, every), P(every, None), P(every))
    return jax.shard_map(
        body, mesh=fine, in_specs=placed, out_specs=P(None, every), check_vma=False
    )
```

```python
import jax
import jax.numpy as jnp
from jax import lax
from jax.experimental import pallas as pl
from jax.experimental.pallas import tpu as pltpu
from jax.sharding import Mesh, PartitionSpec as P

F32 = jnp.float32
BF16 = jnp.bfloat16
TILE = 256
SMALL = pltpu.CompilerParams(vmem_limit_bytes=16 * 1024 * 1024)


def split(x):
    high = x.astype(BF16)
    return high, (x - high.astype(F32)).astype(BF16)


def hot(mask):
    return jnp.where(mask, 1.0, 0.0).astype(BF16)


def rows_of(shape):
    return lax.broadcasted_iota(jnp.int32, shape, 0)


def lane_tile(ref, row, t):
    return ref[row : row + 1, t * TILE : (t + 1) * TILE]


def fraction_of(offsets):
    return (offsets.astype(F32) + 0.5) / 1024.0


def two_weights(index, frac, place):
    lower = place == index
    upper = place == index + 1
    weight = jnp.where(lower, 1.0 - frac, jnp.where(upper, frac, 0.0))
    slope = jnp.where(upper, 1.0, jnp.where(lower, -1.0, 0.0))
    return weight, slope


def with_next_x(block):
    return block, pltpu.roll(block, block.shape[1] - 1, 1) - block


def count_earlier(owner_row):
    num_rows = owner_row.shape[1]
    chunks = num_rows // 128
    names = owner_row.astype(F32)
    columns = jnp.concatenate([names[:, i * 128 : (i + 1) * 128] for i in range(chunks)], 0)
    columns = jnp.concatenate([columns, jnp.zeros((128 - chunks, 128), F32)], 0).T
    earlier = rows_of((128, 128)) < lax.broadcasted_iota(jnp.int32, (128, 128), 1)
    counts = [jnp.zeros((8, 128), F32)] * chunks
    for i in range(chunks):
        column = jnp.broadcast_to(columns[:, i : i + 1], (128, 128))
        for j in range(i, chunks):
            same = column == names[:, j * 128 : (j + 1) * 128]
            if i == j:
                same = same & earlier
            ones = jnp.where(same, 1.0, 0.0)
            counts[j] = counts[j] + jnp.sum(ones.reshape(16, 8, 128), axis=0)
    return jnp.concatenate([jnp.sum(c, axis=0, keepdims=True) for c in counts], 1)


def faces_kernel(grid_ref, face_z_ref, face_y_ref, edge_ref):
    block_z, block_y = face_y_ref.shape[0], face_z_ref.shape[0]
    face_z_ref[...] = grid_ref[:block_y]
    edge_ref[...] = grid_ref[:1]
    for z in range(block_z):
        face_y_ref[z : z + 1] = grid_ref[z * block_y : z * block_y + 1]


def read_tiles(lhs_ref, cells_ref, offsets_ref, grad_ref):
    rows, size_x = lhs_ref.shape[0] // 2, lhs_ref.shape[1] // 2
    for t in range(cells_ref.shape[1] // TILE):
        at_x = hot(rows_of((size_x, TILE)) == lane_tile(cells_ref, 2, t))
        read = jnp.dot(lhs_ref[...], jnp.concatenate([at_x, at_x], 0), preferred_element_type=F32)
        frac = [fraction_of(lane_tile(offsets_ref, a, t)) for a in range(3)]
        index_z = jnp.broadcast_to(lane_tile(cells_ref, 0, t) & 15, (16, TILE))
        index_y = lane_tile(cells_ref, 1, t) & 15
        value = [jnp.zeros((16, TILE), F32)] * 2
        diff = [jnp.zeros((16, TILE), F32)] * 2
        for z in range(16):
            value_z = read[z * 16 : (z + 1) * 16]
            diff_z = read[rows + z * 16 : rows + (z + 1) * 16]
            for side in range(2):
                if z < side:
                    continue
                here = index_z == z - side
                value[side] = jnp.where(here, value_z, value[side])
                diff[side] = jnp.where(here, diff_z, diff[side])
        low = value[0] + diff[0] * frac[2]
        high = value[1] + diff[1] * frac[2]
        weight_y, slope_y = two_weights(index_y, frac[1], rows_of((16, TILE)))
        parts = [
            (high - low) * weight_y,
            (low * (1.0 - frac[0]) + high * frac[0]) * slope_y,
            (diff[0] * (1.0 - frac[0]) + diff[1] * frac[0]) * weight_y,
        ]
        sums = [jnp.sum(p, axis=0, keepdims=True) for p in parts]
        lanes = slice(t * TILE, (t + 1) * TILE)
        grad_ref[:, lanes] = jnp.concatenate(sums + [jnp.zeros((5, TILE), F32)], 0)


def inner_kernel(grid_ref, cells_ref, offsets_ref, owners_ref, grad_ref, place_ref, lhs_ref):
    rows, size_x = grid_ref.shape
    for part, block in enumerate(with_next_x(grid_ref[...])):
        for half, piece in enumerate(split(block)):
            lhs_ref[part * rows : (part + 1) * rows, half * size_x : (half + 1) * size_x] = piece
    owners = owners_ref[...]
    rank = count_earlier(owners).astype(jnp.int32)
    place_ref[...] = ((owners >> 1) & 31) * 4 + rank
    read_tiles(lhs_ref, cells_ref, offsets_ref, grad_ref)


def send_kernel(
    face_z_ref, face_y_ref, edge_ref, grad_ref, place_ref, cells_ref, offsets_ref, owners_ref,
    slots_ref, send_ref, halo_ref, value_ref, hot_ref,
):
    size_x = edge_ref.shape[1]
    edge = jnp.broadcast_to(edge_ref[...], (8, size_x))
    halo = jnp.concatenate([face_z_ref[...], face_y_ref[...], edge], 0)
    count = halo.shape[0]
    for part, block in enumerate(with_next_x(halo)):
        for half, piece in enumerate(split(block)):
            halo_ref[(2 * half + part) * count : (2 * half + part + 1) * count, :] = piece
    for t in range(cells_ref.shape[1] // TILE):
        lanes = slice(t * TILE, (t + 1) * TILE)
        at_x = hot(rows_of((size_x, TILE)) == lane_tile(cells_ref, 2, t))
        read = jnp.dot(halo_ref[...], at_x, preferred_element_type=F32)
        read = read[: 2 * count] + read[2 * count :]
        frac = [fraction_of(lane_tile(offsets_ref, a, t)) for a in range(3)]
        index_z = lane_tile(cells_ref, 0, t) & 15
        index_y = lane_tile(cells_ref, 1, t) & 15
        diff = read[count:]
        value = read[:count] + diff * frac[2]
        weight_z, slope_z = two_weights(index_z, frac[0], rows_of((16, TILE)))
        weight_y, slope_y = two_weights(index_y, frac[1], rows_of((16, TILE)))
        top_z, step_z = two_weights(index_z, frac[0], 16)
        top_y, step_y = two_weights(index_y, frac[1], 16)

        def over(block, weight):
            return jnp.sum(block * weight, axis=0, keepdims=True)

        on_z, on_y, on_edge = value[:16], value[16:32], value[32:33]
        dif_z, dif_y, dif_edge = diff[:16], diff[16:32], diff[32:33]
        grad_z = step_z * (over(on_z, weight_y) + top_y * on_edge) + top_y * over(on_y, slope_z)
        grad_y = top_z * (over(on_z, slope_y) + step_y * on_edge) + step_y * over(on_y, weight_z)
        grad_x = top_z * (over(dif_z, weight_y) + top_y * dif_edge) + top_y * over(dif_y, weight_z)
        grad_z = grad_z + grad_ref[0:1, lanes]
        grad_y = grad_y + grad_ref[1:2, lanes]
        grad_x = grad_x + grad_ref[2:3, lanes]
        slot = slots_ref[:, lanes].astype(F32)
        kind = rows_of((8, TILE)) & 3
        four = jnp.where(
            kind == 0, grad_z, jnp.where(kind == 1, grad_y, jnp.where(kind == 2, grad_x, slot))
        )
        owners = owners_ref[:, lanes]
        here = (rows_of((128, TILE)) >> 2) == (owners >> 6) * 2 + (owners & 1)
        for half, piece in enumerate(split(four)):
            tall = jnp.concatenate([piece.astype(F32)] * 16, 0)
            value_ref[half * 128 : (half + 1) * 128, lanes] = jnp.where(here, tall, 0.0).astype(BF16)
        hot_ref[:, lanes] = hot(rows_of((128, TILE)) == place_ref[:, lanes])
    both = lax.dot_general(
        value_ref[...], hot_ref[...], (((1,), (1,)), ((), ())), preferred_element_type=F32
    )
    send_ref[...] = both[:128] + both[128:]


def turn_kernel(in_ref, out_ref):
    out_ref[...] = in_ref[...].T


def place_kernel(recv_ref, out_ref, value_ref, hot_ref):
    turned = recv_ref[...].T
    high, low = split(turned)
    halves = (high.astype(F32), low.astype(F32))
    for j in range(32):
        lanes = slice(j * 128, (j + 1) * 128)
        slot = turned[4 * j + 3 : 4 * j + 4].astype(jnp.int32)
        here = (rows_of((64, 128)) >> 2) == (slot >> 7)
        for half, piece in enumerate(halves):
            four = piece[4 * j : 4 * j + 4]
            eight = jnp.concatenate([four, four], 0)
            tall = jnp.concatenate([eight] * 8, 0)
            value_ref[half * 64 : (half + 1) * 64, lanes] = jnp.where(here, tall, 0.0).astype(BF16)
        hot_ref[:, lanes] = hot(rows_of((128, 128)) == (slot & 127))
    both = lax.dot_general(
        value_ref[...], hot_ref[...], (((1,), (1,)), ((), ())), preferred_element_type=F32
    )
    total = both[:64] + both[64:]
    for h in range(16):
        out_ref[:, h * 128 : (h + 1) * 128] = total[4 * h : 4 * h + 3]


def run_faces(plane, block_z, block_y):
    size_x = plane.shape[1]
    return pl.pallas_call(
        faces_kernel,
        out_shape=(
            jax.ShapeDtypeStruct((block_y, size_x), F32),
            jax.ShapeDtypeStruct((block_z, size_x), F32),
            jax.ShapeDtypeStruct((1, size_x), F32),
        ),
        compiler_params=SMALL,
        name="faces",
    )(plane)


def run_inner(plane, cells, offsets, owner_row):
    rows, size_x = plane.shape
    num_rows = cells.shape[1]
    return pl.pallas_call(
        inner_kernel,
        out_shape=(
            jax.ShapeDtypeStruct((8, num_rows), F32),
            jax.ShapeDtypeStruct((1, num_rows), jnp.int32),
        ),
        scratch_shapes=[pltpu.VMEM((2 * rows, 2 * size_x), BF16)],
        compiler_params=SMALL,
        cost_estimate=pl.CostEstimate(
            flops=8 * rows * size_x * num_rows, bytes_accessed=1000000, transcendentals=0
        ),
        name="inner",
    )(plane, cells, offsets, owner_row)


def run_send(face_z, face_y, edge, grad, place, cells, offsets, owner_row, slot_row):
    num_rows = cells.shape[1]
    return pl.pallas_call(
        send_kernel,
        out_shape=jax.ShapeDtypeStruct((128, 128), F32),
        scratch_shapes=[
            pltpu.VMEM((160, edge.shape[1]), BF16),
            pltpu.VMEM((256, num_rows), BF16),
            pltpu.VMEM((128, num_rows), BF16),
        ],
        compiler_params=SMALL,
        name="send",
    )(face_z, face_y, edge, grad, place, cells, offsets, owner_row, slot_row)


def run_turn(x):
    return pl.pallas_call(
        turn_kernel,
        out_shape=jax.ShapeDtypeStruct((128, 128), F32),
        compiler_params=SMALL,
        name="turn",
    )(x)


def run_place(received, num_rows):
    return pl.pallas_call(
        place_kernel,
        out_shape=jax.ShapeDtypeStruct((3, num_rows), F32),
        scratch_shapes=[pltpu.VMEM((128, 4096), BF16), pltpu.VMEM((128, 4096), BF16)],
        compiler_params=SMALL,
        name="place",
    )(received)


def body(grid_grad, cells, offsets, owners, slots):
    block_z, block_y, size_x = grid_grad.shape
    num_rows = cells.shape[1]
    count_z = lax.axis_size("gz")
    count_y = lax.axis_size("z") * lax.axis_size("c")
    next_z = [((i + 1) % count_z, i) for i in range(count_z)]
    next_y = [((i + 1) % count_y, i) for i in range(count_y)]
    next_zy = [
        (sz * count_y + sy, dz * count_y + dy) for sz, dz in next_z for sy, dy in next_y
    ]
    plane = grid_grad.reshape(block_z * block_y, size_x)
    face_z, face_y, edge = run_faces(plane, block_z, block_y)
    face_z = lax.ppermute(face_z, "gz", next_z)
    face_y = lax.ppermute(face_y, ("z", "c"), next_y)
    edge = lax.ppermute(edge, ("gz", "z", "c"), next_zy)
    owner_row = owners.reshape(1, num_rows)
    slot_row = slots.reshape(1, num_rows)
    grad, place = run_inner(plane, cells, offsets, owner_row)
    send = run_send(face_z, face_y, edge, grad, place, cells, offsets, owner_row, slot_row)
    in_plane = lax.all_to_all(send, ("gz", "c"), 0, 0, tiled=True)
    received = lax.all_to_all(run_turn(in_plane), "z", 0, 0, tiled=True)
    return run_place(received, num_rows)


def solution(mesh):
    fine = Mesh(mesh.devices.reshape(16, 32, 2), ("gz", "z", "c"))
    every = ("gz", "z", "c")
    placed = (P("gz", ("z", "c"), None), P(None, every), P(None, every), P(every, None), P(every))
    return jax.shard_map(
        body, mesh=fine, in_specs=placed, out_specs=P(None, every), check_vma=False
    )
```

```python
import jax
import jax.numpy as jnp
from jax import lax
from jax.experimental import pallas as pl
from jax.experimental.pallas import tpu as pltpu
from jax.sharding import Mesh, PartitionSpec as P

F32 = jnp.float32
BF16 = jnp.bfloat16
TILE = 256
SMALL = pltpu.CompilerParams(vmem_limit_bytes=16 * 1024 * 1024)


def split(x):
    high = x.astype(BF16)
    return high, (x - high.astype(F32)).astype(BF16)


def rows_of(shape):
    return lax.broadcasted_iota(jnp.int32, shape, 0)


def hot_rows(shape, place):
    narrow = jnp.broadcast_to(place.astype(jnp.int16), shape)
    one = jnp.ones(shape, BF16)
    return jnp.where(rows_of(shape).astype(jnp.int16) == narrow, one, jnp.zeros(shape, BF16))


def lane_tile(ref, row, t):
    return ref[row : row + 1, t * TILE : (t + 1) * TILE]


def fraction_of(offsets):
    return (offsets.astype(F32) + 0.5) / 1024.0


def two_weights(index, frac, place):
    lower = place == index
    upper = place == index + 1
    weight = jnp.where(lower, 1.0 - frac, jnp.where(upper, frac, 0.0))
    slope = jnp.where(upper, 1.0, jnp.where(lower, -1.0, 0.0))
    return weight, slope


def with_next_x(block):
    return block, pltpu.roll(block, block.shape[1] - 1, 1) - block


def count_earlier(owner_row):
    num_rows = owner_row.shape[1]
    chunks = num_rows // 128
    names = owner_row.astype(F32)
    columns = jnp.concatenate([names[:, i * 128 : (i + 1) * 128] for i in range(chunks)], 0)
    columns = jnp.concatenate([columns, jnp.zeros((128 - chunks, 128), F32)], 0).T
    earlier = rows_of((128, 128)) < lax.broadcasted_iota(jnp.int32, (128, 128), 1)
    counts = [jnp.zeros((8, 128), F32)] * chunks
    for i in range(chunks):
        column = jnp.broadcast_to(columns[:, i : i + 1], (128, 128))
        for j in range(i, chunks):
            same = column == names[:, j * 128 : (j + 1) * 128]
            if i == j:
                same = same & earlier
            ones = jnp.where(same, 1.0, 0.0)
            counts[j] = counts[j] + jnp.sum(ones.reshape(16, 8, 128), axis=0)
    return jnp.concatenate([jnp.sum(c, axis=0, keepdims=True) for c in counts], 1)


def faces_kernel(grid_ref, face_z_ref, face_y_ref, edge_ref):
    block_z, block_y = face_y_ref.shape[0], face_z_ref.shape[0]
    face_z_ref[...] = grid_ref[:block_y]
    edge_ref[...] = grid_ref[:1]
    for z in range(block_z):
        face_y_ref[z : z + 1] = grid_ref[z * block_y : z * block_y + 1]


def read_tiles(lhs_ref, cells_ref, offsets_ref, grad_ref):
    rows, size_x = lhs_ref.shape[0] // 2, lhs_ref.shape[1] // 2
    for t in range(cells_ref.shape[1] // TILE):
        at_x = hot_rows((size_x, TILE), lane_tile(cells_ref, 2, t))
        read = jnp.dot(lhs_ref[...], jnp.concatenate([at_x, at_x], 0), preferred_element_type=F32)
        frac = [fraction_of(lane_tile(offsets_ref, a, t)) for a in range(3)]
        index_z = jnp.broadcast_to(lane_tile(cells_ref, 0, t) & 15, (16, TILE))
        index_y = lane_tile(cells_ref, 1, t) & 15
        value = [jnp.zeros((16, TILE), F32)] * 2
        diff = [jnp.zeros((16, TILE), F32)] * 2
        for z in range(16):
            value_z = read[z * 16 : (z + 1) * 16]
            diff_z = read[rows + z * 16 : rows + (z + 1) * 16]
            for side in range(2):
                if z < side:
                    continue
                here = index_z == z - side
                value[side] = jnp.where(here, value_z, value[side])
                diff[side] = jnp.where(here, diff_z, diff[side])
        low = value[0] + diff[0] * frac[2]
        high = value[1] + diff[1] * frac[2]
        weight_y, slope_y = two_weights(index_y, frac[1], rows_of((16, TILE)))
        parts = [
            (high - low) * weight_y,
            (low * (1.0 - frac[0]) + high * frac[0]) * slope_y,
            (diff[0] * (1.0 - frac[0]) + diff[1] * frac[0]) * weight_y,
        ]
        sums = [jnp.sum(p, axis=0, keepdims=True) for p in parts]
        lanes = slice(t * TILE, (t + 1) * TILE)
        grad_ref[:, lanes] = jnp.concatenate(sums + [jnp.zeros((5, TILE), F32)], 0)


def inner_kernel(grid_ref, cells_ref, offsets_ref, owners_ref, grad_ref, place_ref, lhs_ref):
    rows, size_x = grid_ref.shape
    for part, block in enumerate(with_next_x(grid_ref[...])):
        for half, piece in enumerate(split(block)):
            lhs_ref[part * rows : (part + 1) * rows, half * size_x : (half + 1) * size_x] = piece
    owners = owners_ref[...]
    rank = count_earlier(owners).astype(jnp.int32)
    place_ref[...] = ((owners >> 1) & 31) * 4 + rank
    read_tiles(lhs_ref, cells_ref, offsets_ref, grad_ref)


def send_kernel(
    face_z_ref, face_y_ref, edge_ref, grad_ref, place_ref, cells_ref, offsets_ref, owners_ref,
    slots_ref, send_ref, halo_ref, value_ref, hot_ref,
):
    size_x = edge_ref.shape[1]
    edge = jnp.broadcast_to(edge_ref[...], (8, size_x))
    halo = jnp.concatenate([face_z_ref[...], face_y_ref[...], edge], 0)
    count = halo.shape[0]
    for part, block in enumerate(with_next_x(halo)):
        for half, piece in enumerate(split(block)):
            halo_ref[(2 * half + part) * count : (2 * half + part + 1) * count, :] = piece
    for t in range(cells_ref.shape[1] // TILE):
        lanes = slice(t * TILE, (t + 1) * TILE)
        at_x = hot_rows((size_x, TILE), lane_tile(cells_ref, 2, t))
        read = jnp.dot(halo_ref[...], at_x, preferred_element_type=F32)
        read = read[: 2 * count] + read[2 * count :]
        frac = [fraction_of(lane_tile(offsets_ref, a, t)) for a in range(3)]
        index_z = lane_tile(cells_ref, 0, t) & 15
        index_y = lane_tile(cells_ref, 1, t) & 15
        diff = read[count:]
        value = read[:count] + diff * frac[2]
        weight_z, slope_z = two_weights(index_z, frac[0], rows_of((16, TILE)))
        weight_y, slope_y = two_weights(index_y, frac[1], rows_of((16, TILE)))
        top_z, step_z = two_weights(index_z, frac[0], 16)
        top_y, step_y = two_weights(index_y, frac[1], 16)

        def over(block, weight):
            return jnp.sum(block * weight, axis=0, keepdims=True)

        on_z, on_y, on_edge = value[:16], value[16:32], value[32:33]
        dif_z, dif_y, dif_edge = diff[:16], diff[16:32], diff[32:33]
        grad_z = step_z * (over(on_z, weight_y) + top_y * on_edge) + top_y * over(on_y, slope_z)
        grad_y = top_z * (over(on_z, slope_y) + step_y * on_edge) + step_y * over(on_y, weight_z)
        grad_x = top_z * (over(dif_z, weight_y) + top_y * dif_edge) + top_y * over(dif_y, weight_z)
        grad_z = grad_z + grad_ref[0:1, lanes]
        grad_y = grad_y + grad_ref[1:2, lanes]
        grad_x = grad_x + grad_ref[2:3, lanes]
        slot = slots_ref[:, lanes].astype(F32)
        kind = rows_of((8, TILE)) & 3
        four = jnp.where(
            kind == 0, grad_z, jnp.where(kind == 1, grad_y, jnp.where(kind == 2, grad_x, slot))
        )
        owners = owners_ref[:, lanes]
        here = (rows_of((128, TILE)) >> 2) == (owners >> 6) * 2 + (owners & 1)
        for half, piece in enumerate(split(four)):
            tall = jnp.concatenate([piece.astype(F32)] * 16, 0)
            value_ref[half * 128 : (half + 1) * 128, lanes] = jnp.where(here, tall, 0.0).astype(BF16)
        hot_ref[:, lanes] = hot_rows((128, TILE), place_ref[:, lanes])
    both = lax.dot_general(
        value_ref[...], hot_ref[...], (((1,), (1,)), ((), ())), preferred_element_type=F32
    )
    send_ref[...] = both[:128] + both[128:]


def turn_kernel(in_ref, out_ref):
    out_ref[...] = in_ref[...].T


def place_kernel(recv_ref, out_ref, value_ref, hot_ref):
    turned = recv_ref[...].T
    high, low = split(turned)
    halves = (high.astype(F32), low.astype(F32))
    for j in range(32):
        lanes = slice(j * 128, (j + 1) * 128)
        slot = turned[4 * j + 3 : 4 * j + 4].astype(jnp.int32)
        here = (rows_of((64, 128)) >> 2) == (slot >> 7)
        for half, piece in enumerate(halves):
            four = piece[4 * j : 4 * j + 4]
            eight = jnp.concatenate([four, four], 0)
            tall = jnp.concatenate([eight] * 8, 0)
            value_ref[half * 64 : (half + 1) * 64, lanes] = jnp.where(here, tall, 0.0).astype(BF16)
        hot_ref[:, lanes] = hot_rows((128, 128), slot & 127)
    both = lax.dot_general(
        value_ref[...], hot_ref[...], (((1,), (1,)), ((), ())), preferred_element_type=F32
    )
    total = both[:64] + both[64:]
    for h in range(16):
        out_ref[:, h * 128 : (h + 1) * 128] = total[4 * h : 4 * h + 3]


def run_faces(plane, block_z, block_y):
    size_x = plane.shape[1]
    return pl.pallas_call(
        faces_kernel,
        out_shape=(
            jax.ShapeDtypeStruct((block_y, size_x), F32),
            jax.ShapeDtypeStruct((block_z, size_x), F32),
            jax.ShapeDtypeStruct((1, size_x), F32),
        ),
        compiler_params=SMALL,
        name="faces",
    )(plane)


def run_inner(plane, cells, offsets, owner_row):
    rows, size_x = plane.shape
    num_rows = cells.shape[1]
    return pl.pallas_call(
        inner_kernel,
        out_shape=(
            jax.ShapeDtypeStruct((8, num_rows), F32),
            jax.ShapeDtypeStruct((1, num_rows), jnp.int32),
        ),
        scratch_shapes=[pltpu.VMEM((2 * rows, 2 * size_x), BF16)],
        compiler_params=SMALL,
        cost_estimate=pl.CostEstimate(
            flops=8 * rows * size_x * num_rows, bytes_accessed=1000000, transcendentals=0
        ),
        name="inner",
    )(plane, cells, offsets, owner_row)


def run_send(face_z, face_y, edge, grad, place, cells, offsets, owner_row, slot_row):
    num_rows = cells.shape[1]
    return pl.pallas_call(
        send_kernel,
        out_shape=jax.ShapeDtypeStruct((128, 128), F32),
        scratch_shapes=[
            pltpu.VMEM((160, edge.shape[1]), BF16),
            pltpu.VMEM((256, num_rows), BF16),
            pltpu.VMEM((128, num_rows), BF16),
        ],
        compiler_params=SMALL,
        name="send",
    )(face_z, face_y, edge, grad, place, cells, offsets, owner_row, slot_row)


def run_turn(x):
    return pl.pallas_call(
        turn_kernel,
        out_shape=jax.ShapeDtypeStruct((128, 128), F32),
        compiler_params=SMALL,
        name="turn",
    )(x)


def run_place(received, num_rows):
    return pl.pallas_call(
        place_kernel,
        out_shape=jax.ShapeDtypeStruct((3, num_rows), F32),
        scratch_shapes=[pltpu.VMEM((128, 4096), BF16), pltpu.VMEM((128, 4096), BF16)],
        compiler_params=SMALL,
        name="place",
    )(received)


def body(grid_grad, cells, offsets, owners, slots):
    block_z, block_y, size_x = grid_grad.shape
    num_rows = cells.shape[1]
    count_z = lax.axis_size("gz")
    count_y = lax.axis_size("z") * lax.axis_size("c")
    next_z = [((i + 1) % count_z, i) for i in range(count_z)]
    next_y = [((i + 1) % count_y, i) for i in range(count_y)]
    next_zy = [
        (sz * count_y + sy, dz * count_y + dy) for sz, dz in next_z for sy, dy in next_y
    ]
    plane = grid_grad.reshape(block_z * block_y, size_x)
    face_z, face_y, edge = run_faces(plane, block_z, block_y)
    face_z = lax.ppermute(face_z, "gz", next_z)
    face_y = lax.ppermute(face_y, ("z", "c"), next_y)
    edge = lax.ppermute(edge, ("gz", "z", "c"), next_zy)
    owner_row = owners.reshape(1, num_rows)
    slot_row = slots.reshape(1, num_rows)
    grad, place = run_inner(plane, cells, offsets, owner_row)
    send = run_send(face_z, face_y, edge, grad, place, cells, offsets, owner_row, slot_row)
    in_plane = lax.all_to_all(send, ("gz", "c"), 0, 0, tiled=True)
    received = lax.all_to_all(run_turn(in_plane), "z", 0, 0, tiled=True)
    return run_place(received, num_rows)


def solution(mesh):
    fine = Mesh(mesh.devices.reshape(16, 32, 2), ("gz", "z", "c"))
    every = ("gz", "z", "c")
    placed = (P("gz", ("z", "c"), None), P(None, every), P(None, every), P(every, None), P(every))
    return jax.shard_map(
        body, mesh=fine, in_specs=placed, out_specs=P(None, every), check_vma=False
    )
```

```python
import jax
import jax.numpy as jnp
from jax import lax
from jax.experimental import pallas as pl
from jax.experimental.pallas import tpu as pltpu
from jax.sharding import Mesh, PartitionSpec as P


F32 = jnp.float32
BF16 = jnp.bfloat16
TILE = 256
SMALL = pltpu.CompilerParams(vmem_limit_bytes=16 * 1024 * 1024)


def split(x):
    high = x.astype(BF16)
    return high, (x - high.astype(F32)).astype(BF16)


def rows_of(shape):
    return lax.broadcasted_iota(jnp.int32, shape, 0)


def hot_rows(shape, place):
    narrow = jnp.broadcast_to(place.astype(jnp.int16), shape)
    one = jnp.ones(shape, BF16)
    return jnp.where(rows_of(shape).astype(jnp.int16) == narrow, one, jnp.zeros(shape, BF16))


def lane_tile(ref, row, t):
    return ref[row : row + 1, t * TILE : (t + 1) * TILE]


def fraction_of(offsets):
    return (offsets.astype(F32) + 0.5) / 1024.0


def two_weights(index, frac, place):
    lower = place == index
    upper = place == index + 1
    weight = jnp.where(lower, 1.0 - frac, jnp.where(upper, frac, 0.0))
    slope = jnp.where(upper, 1.0, jnp.where(lower, -1.0, 0.0))
    return weight, slope


def with_next_x(block):
    return block, pltpu.roll(block, block.shape[1] - 1, 1) - block


def count_earlier(owner_row):
    num_rows = owner_row.shape[1]
    chunks = num_rows // 128
    names = owner_row.astype(F32)
    columns = jnp.concatenate([names[:, i * 128 : (i + 1) * 128] for i in range(chunks)], 0)
    columns = jnp.concatenate([columns, jnp.zeros((128 - chunks, 128), F32)], 0).T
    earlier = rows_of((128, 128)) < lax.broadcasted_iota(jnp.int32, (128, 128), 1)
    counts = [jnp.zeros((8, 128), F32)] * chunks
    for i in range(chunks):
        column = jnp.broadcast_to(columns[:, i : i + 1], (128, 128))
        for j in range(i, chunks):
            same = column == names[:, j * 128 : (j + 1) * 128]
            if i == j:
                same = same & earlier
            ones = jnp.where(same, 1.0, 0.0)
            counts[j] = counts[j] + jnp.sum(ones.reshape(16, 8, 128), axis=0)
    return jnp.concatenate([jnp.sum(c, axis=0, keepdims=True) for c in counts], 1)


def edge_kernel(face_z_ref, edge_ref):
    edge_ref[...] = face_z_ref[:1]


def face_y_kernel(grid_ref, face_y_ref):
    block_z = face_y_ref.shape[0]
    block_y = grid_ref.shape[0] // block_z
    for z in range(block_z):
        face_y_ref[z : z + 1] = grid_ref[z * block_y : z * block_y + 1]


def read_tiles(lhs_ref, cells_ref, offsets_ref, grad_ref):
    rows, size_x = lhs_ref.shape[0] // 2, lhs_ref.shape[1] // 2
    for t in range(cells_ref.shape[1] // TILE):
        at_x = hot_rows((size_x, TILE), lane_tile(cells_ref, 2, t))
        read = jnp.dot(lhs_ref[...], jnp.concatenate([at_x, at_x], 0), preferred_element_type=F32)
        frac = [fraction_of(lane_tile(offsets_ref, a, t)) for a in range(3)]
        index_z = jnp.broadcast_to(lane_tile(cells_ref, 0, t) & 15, (16, TILE))
        index_y = lane_tile(cells_ref, 1, t) & 15
        value = [jnp.zeros((16, TILE), F32)] * 2
        diff = [jnp.zeros((16, TILE), F32)] * 2
        for z in range(16):
            value_z = read[z * 16 : (z + 1) * 16]
            diff_z = read[rows + z * 16 : rows + (z + 1) * 16]
            for side in range(2):
                if z < side:
                    continue
                here = index_z == z - side
                value[side] = jnp.where(here, value_z, value[side])
                diff[side] = jnp.where(here, diff_z, diff[side])
        low = value[0] + diff[0] * frac[2]
        high = value[1] + diff[1] * frac[2]
        weight_y, slope_y = two_weights(index_y, frac[1], rows_of((16, TILE)))
        parts = [
            (high - low) * weight_y,
            (low * (1.0 - frac[0]) + high * frac[0]) * slope_y,
            (diff[0] * (1.0 - frac[0]) + diff[1] * frac[0]) * weight_y,
        ]
        sums = [jnp.sum(p, axis=0, keepdims=True) for p in parts]
        lanes = slice(t * TILE, (t + 1) * TILE)
        grad_ref[:, lanes] = jnp.concatenate(sums + [jnp.zeros((5, TILE), F32)], 0)


def inner_kernel(grid_ref, cells_ref, offsets_ref, owners_ref, grad_ref, place_ref, lhs_ref):
    rows, size_x = grid_ref.shape
    for part, block in enumerate(with_next_x(grid_ref[...])):
        for half, piece in enumerate(split(block)):
            lhs_ref[part * rows : (part + 1) * rows, half * size_x : (half + 1) * size_x] = piece
    owners = owners_ref[...]
    rank = count_earlier(owners).astype(jnp.int32)
    place_ref[...] = ((owners >> 1) & 31) * 4 + rank
    read_tiles(lhs_ref, cells_ref, offsets_ref, grad_ref)


def send_kernel(
    face_z_ref, face_y_ref, edge_ref, grad_ref, place_ref, cells_ref, offsets_ref, owners_ref,
    slots_ref, send_ref, halo_ref, value_ref, hot_ref,
):
    size_x = edge_ref.shape[1]
    edge = jnp.broadcast_to(edge_ref[...], (8, size_x))
    halo = jnp.concatenate([face_z_ref[...], face_y_ref[...], edge], 0)
    count = halo.shape[0]
    for part, block in enumerate(with_next_x(halo)):
        for half, piece in enumerate(split(block)):
            halo_ref[(2 * half + part) * count : (2 * half + part + 1) * count, :] = piece
    for t in range(cells_ref.shape[1] // TILE):
        lanes = slice(t * TILE, (t + 1) * TILE)
        at_x = hot_rows((size_x, TILE), lane_tile(cells_ref, 2, t))
        read = jnp.dot(halo_ref[...], at_x, preferred_element_type=F32)
        read = read[: 2 * count] + read[2 * count :]
        frac = [fraction_of(lane_tile(offsets_ref, a, t)) for a in range(3)]
        index_z = lane_tile(cells_ref, 0, t) & 15
        index_y = lane_tile(cells_ref, 1, t) & 15
        diff = read[count:]
        value = read[:count] + diff * frac[2]
        weight_z, slope_z = two_weights(index_z, frac[0], rows_of((16, TILE)))
        weight_y, slope_y = two_weights(index_y, frac[1], rows_of((16, TILE)))
        top_z, step_z = two_weights(index_z, frac[0], 16)
        top_y, step_y = two_weights(index_y, frac[1], 16)

        def over(block, weight):
            return jnp.sum(block * weight, axis=0, keepdims=True)

        on_z, on_y, on_edge = value[:16], value[16:32], value[32:33]
        dif_z, dif_y, dif_edge = diff[:16], diff[16:32], diff[32:33]
        grad_z = step_z * (over(on_z, weight_y) + top_y * on_edge) + top_y * over(on_y, slope_z)
        grad_y = top_z * (over(on_z, slope_y) + step_y * on_edge) + step_y * over(on_y, weight_z)
        grad_x = top_z * (over(dif_z, weight_y) + top_y * dif_edge) + top_y * over(dif_y, weight_z)
        grad_z = grad_z + grad_ref[0:1, lanes]
        grad_y = grad_y + grad_ref[1:2, lanes]
        grad_x = grad_x + grad_ref[2:3, lanes]
        slot = slots_ref[:, lanes].astype(F32)
        kind = rows_of((8, TILE)) & 3
        four = jnp.where(
            kind == 0, grad_z, jnp.where(kind == 1, grad_y, jnp.where(kind == 2, grad_x, slot))
        )
        owners = owners_ref[:, lanes]
        here = (rows_of((128, TILE)) >> 2) == (owners >> 6) * 2 + (owners & 1)
        for half, piece in enumerate(split(four)):
            tall = jnp.concatenate([piece.astype(F32)] * 16, 0)
            value_ref[half * 128 : (half + 1) * 128, lanes] = jnp.where(here, tall, 0.0).astype(BF16)
        hot_ref[:, lanes] = hot_rows((128, TILE), place_ref[:, lanes])
    both = lax.dot_general(
        value_ref[...], hot_ref[...], (((1,), (1,)), ((), ())), preferred_element_type=F32
    )
    send_ref[...] = both[:128] + both[128:]


def turn_kernel(in_ref, out_ref):
    out_ref[...] = in_ref[...].T


def place_kernel(recv_ref, out_ref, value_ref, hot_ref):
    turned = recv_ref[...].T
    high, low = split(turned)
    halves = (high.astype(F32), low.astype(F32))
    for j in range(32):
        lanes = slice(j * 128, (j + 1) * 128)
        slot = turned[4 * j + 3 : 4 * j + 4].astype(jnp.int32)
        here = (rows_of((64, 128)) >> 2) == (slot >> 7)
        for half, piece in enumerate(halves):
            four = piece[4 * j : 4 * j + 4]
            eight = jnp.concatenate([four, four], 0)
            tall = jnp.concatenate([eight] * 8, 0)
            value_ref[half * 64 : (half + 1) * 64, lanes] = jnp.where(here, tall, 0.0).astype(BF16)
        hot_ref[:, lanes] = hot_rows((128, 128), slot & 127)
    both = lax.dot_general(
        value_ref[...], hot_ref[...], (((1,), (1,)), ((), ())), preferred_element_type=F32
    )
    total = both[:64] + both[64:]
    for h in range(16):
        out_ref[:, h * 128 : (h + 1) * 128] = total[4 * h : 4 * h + 3]


def run_edge(face_z):
    return pl.pallas_call(
        edge_kernel,
        out_shape=jax.ShapeDtypeStruct((1, face_z.shape[1]), F32),
        compiler_params=SMALL,
        name="edge",
    )(face_z)


def run_face_y(plane, block_z):
    return pl.pallas_call(
        face_y_kernel,
        out_shape=jax.ShapeDtypeStruct((block_z, plane.shape[1]), F32),
        compiler_params=SMALL,
        name="face_y",
    )(plane)


def run_inner(plane, cells, offsets, owner_row):
    rows, size_x = plane.shape
    num_rows = cells.shape[1]
    return pl.pallas_call(
        inner_kernel,
        out_shape=(
            jax.ShapeDtypeStruct((8, num_rows), F32),
            jax.ShapeDtypeStruct((1, num_rows), jnp.int32),
        ),
        scratch_shapes=[pltpu.VMEM((2 * rows, 2 * size_x), BF16)],
        compiler_params=SMALL,
        cost_estimate=pl.CostEstimate(
            flops=8 * rows * size_x * num_rows, bytes_accessed=1000000, transcendentals=0
        ),
        name="inner",
    )(plane, cells, offsets, owner_row)


def run_send(face_z, face_y, edge, grad, place, cells, offsets, owner_row, slot_row):
    num_rows = cells.shape[1]
    return pl.pallas_call(
        send_kernel,
        out_shape=jax.ShapeDtypeStruct((128, 128), F32),
        scratch_shapes=[
            pltpu.VMEM((160, edge.shape[1]), BF16),
            pltpu.VMEM((256, num_rows), BF16),
            pltpu.VMEM((128, num_rows), BF16),
        ],
        compiler_params=SMALL,
        name="send",
    )(face_z, face_y, edge, grad, place, cells, offsets, owner_row, slot_row)


def run_turn(x):
    return pl.pallas_call(
        turn_kernel,
        out_shape=jax.ShapeDtypeStruct((128, 128), F32),
        compiler_params=SMALL,
        name="turn",
    )(x)


def run_place(received, num_rows):
    return pl.pallas_call(
        place_kernel,
        out_shape=jax.ShapeDtypeStruct((3, num_rows), F32),
        scratch_shapes=[pltpu.VMEM((128, 4096), BF16), pltpu.VMEM((128, 4096), BF16)],
        compiler_params=SMALL,
        name="place",
    )(received)


def body(grid_grad, cells, offsets, owners, slots):
    block_z, block_y, size_x = grid_grad.shape
    num_rows = cells.shape[1]
    count_z = lax.axis_size("gz")
    count_y = lax.axis_size("z") * lax.axis_size("c")
    next_z = [((i + 1) % count_z, i) for i in range(count_z)]
    next_y = [((i + 1) % count_y, i) for i in range(count_y)]
    next_zy = [
        (sz * count_y + sy, dz * count_y + dy) for sz, dz in next_z for sy, dy in next_y
    ]
    plane = grid_grad.reshape(block_z * block_y, size_x)
    face_z = grid_grad[0]
    edge = run_edge(face_z)
    face_y = run_face_y(plane, block_z)
    face_z = lax.ppermute(face_z, "gz", next_z)
    face_y = lax.ppermute(face_y, ("z", "c"), next_y)
    edge = lax.ppermute(edge, ("gz", "z", "c"), next_zy)
    owner_row = owners.reshape(1, num_rows)
    slot_row = slots.reshape(1, num_rows)
    grad, place = run_inner(plane, cells, offsets, owner_row)
    send = run_send(face_z, face_y, edge, grad, place, cells, offsets, owner_row, slot_row)
    in_plane = lax.all_to_all(send, ("gz", "c"), 0, 0, tiled=True)
    received = lax.all_to_all(run_turn(in_plane), "z", 0, 0, tiled=True)
    return run_place(received, num_rows)


def solution(mesh):
    fine = Mesh(mesh.devices.reshape(16, 32, 2), ("gz", "z", "c"))
    every = ("gz", "z", "c")
    placed = (P("gz", ("z", "c"), None), P(None, every), P(None, every), P(every, None), P(every))
    return jax.shard_map(
        body, mesh=fine, in_specs=placed, out_specs=P(None, every), check_vma=False
    )
```

```python
import jax
import jax.numpy as jnp
from jax import lax
from jax.experimental import pallas as pl
from jax.experimental.pallas import tpu as pltpu
from jax.sharding import Mesh, PartitionSpec as P


F32 = jnp.float32
BF16 = jnp.bfloat16
TILE = 256
SMALL = pltpu.CompilerParams(vmem_limit_bytes=16 * 1024 * 1024)


def split(x):
    high = x.astype(BF16)
    return high, (x - high.astype(F32)).astype(BF16)


def rows_of(shape):
    return lax.broadcasted_iota(jnp.int32, shape, 0)


def hot_rows(shape, place):
    narrow = jnp.broadcast_to(place.astype(jnp.int16), shape)
    one = jnp.ones(shape, BF16)
    return jnp.where(rows_of(shape).astype(jnp.int16) == narrow, one, jnp.zeros(shape, BF16))


def lane_tile(ref, row, t):
    return ref[row : row + 1, t * TILE : (t + 1) * TILE]


def fraction_of(offsets):
    return (offsets.astype(F32) + 0.5) / 1024.0


def two_weights(index, frac, place):
    lower = place == index
    upper = place == index + 1
    weight = jnp.where(lower, 1.0 - frac, jnp.where(upper, frac, 0.0))
    slope = jnp.where(upper, 1.0, jnp.where(lower, -1.0, 0.0))
    return weight, slope


def with_next_x(block):
    return block, pltpu.roll(block, block.shape[1] - 1, 1) - block


def count_earlier(owner_row):
    num_rows = owner_row.shape[1]
    chunks = num_rows // 128
    names = owner_row.astype(F32)
    columns = jnp.concatenate([names[:, i * 128 : (i + 1) * 128] for i in range(chunks)], 0)
    columns = jnp.concatenate([columns, jnp.zeros((128 - chunks, 128), F32)], 0).T
    earlier = rows_of((128, 128)) < lax.broadcasted_iota(jnp.int32, (128, 128), 1)
    counts = [jnp.zeros((8, 128), F32)] * chunks
    for i in range(chunks):
        column = jnp.broadcast_to(columns[:, i : i + 1], (128, 128))
        for j in range(i, chunks):
            same = column == names[:, j * 128 : (j + 1) * 128]
            if i == j:
                same = same & earlier
            ones = jnp.where(same, 1.0, 0.0)
            counts[j] = counts[j] + jnp.sum(ones.reshape(16, 8, 128), axis=0)
    return jnp.concatenate([jnp.sum(c, axis=0, keepdims=True) for c in counts], 1)


def edge_kernel(face_z_ref, edge_ref):
    edge_ref[...] = face_z_ref[:1]


def face_y_kernel(grid_ref, face_y_ref):
    block_z = face_y_ref.shape[0]
    block_y = grid_ref.shape[0] // block_z
    for z in range(block_z):
        face_y_ref[z : z + 1] = grid_ref[z * block_y : z * block_y + 1]


def read_tiles(lhs_ref, cells_ref, offsets_ref, grad_ref):
    rows, size_x = lhs_ref.shape[0] // 2, lhs_ref.shape[1] // 2
    for t in range(cells_ref.shape[1] // TILE):
        at_x = hot_rows((size_x, TILE), lane_tile(cells_ref, 2, t))
        read = jnp.dot(lhs_ref[...], jnp.concatenate([at_x, at_x], 0), preferred_element_type=F32)
        frac = [fraction_of(lane_tile(offsets_ref, a, t)) for a in range(3)]
        index_z = jnp.broadcast_to(lane_tile(cells_ref, 0, t) & 15, (16, TILE))
        index_y = lane_tile(cells_ref, 1, t) & 15
        value = [jnp.zeros((16, TILE), F32)] * 2
        diff = [jnp.zeros((16, TILE), F32)] * 2
        for z in range(16):
            value_z = read[z * 16 : (z + 1) * 16]
            diff_z = read[rows + z * 16 : rows + (z + 1) * 16]
            for side in range(2):
                if z < side:
                    continue
                here = index_z == z - side
                value[side] = jnp.where(here, value_z, value[side])
                diff[side] = jnp.where(here, diff_z, diff[side])
        low = value[0] + diff[0] * frac[2]
        high = value[1] + diff[1] * frac[2]
        weight_y, slope_y = two_weights(index_y, frac[1], rows_of((16, TILE)))
        parts = [
            (high - low) * weight_y,
            (low * (1.0 - frac[0]) + high * frac[0]) * slope_y,
            (diff[0] * (1.0 - frac[0]) + diff[1] * frac[0]) * weight_y,
        ]
        sums = [jnp.sum(p, axis=0, keepdims=True) for p in parts]
        lanes = slice(t * TILE, (t + 1) * TILE)
        grad_ref[:, lanes] = jnp.concatenate(sums + [jnp.zeros((5, TILE), F32)], 0)


def inner_kernel(grid_ref, cells_ref, offsets_ref, owners_ref, grad_ref, hot_ref, lhs_ref):
    rows, size_x = grid_ref.shape
    for part, block in enumerate(with_next_x(grid_ref[...])):
        for half, piece in enumerate(split(block)):
            lhs_ref[part * rows : (part + 1) * rows, half * size_x : (half + 1) * size_x] = piece
    owners = owners_ref[...]
    rank = count_earlier(owners).astype(jnp.int32)
    hot_ref[...] = hot_rows(hot_ref.shape, ((owners >> 1) & 31) * 4 + rank)
    read_tiles(lhs_ref, cells_ref, offsets_ref, grad_ref)


def send_kernel(
    face_z_ref, face_y_ref, edge_ref, grad_ref, hot_ref, cells_ref, offsets_ref, owners_ref,
    slots_ref, send_ref, halo_ref, value_ref,
):
    size_x = edge_ref.shape[1]
    edge = jnp.broadcast_to(edge_ref[...], (8, size_x))
    halo = jnp.concatenate([face_z_ref[...], face_y_ref[...], edge], 0)
    count = halo.shape[0]
    for part, block in enumerate(with_next_x(halo)):
        for half, piece in enumerate(split(block)):
            halo_ref[(2 * half + part) * count : (2 * half + part + 1) * count, :] = piece
    for t in range(cells_ref.shape[1] // TILE):
        lanes = slice(t * TILE, (t + 1) * TILE)
        at_x = hot_rows((size_x, TILE), lane_tile(cells_ref, 2, t))
        read = jnp.dot(halo_ref[...], at_x, preferred_element_type=F32)
        read = read[: 2 * count] + read[2 * count :]
        frac = [fraction_of(lane_tile(offsets_ref, a, t)) for a in range(3)]
        index_z = lane_tile(cells_ref, 0, t) & 15
        index_y = lane_tile(cells_ref, 1, t) & 15
        diff = read[count:]
        value = read[:count] + diff * frac[2]
        weight_z, slope_z = two_weights(index_z, frac[0], rows_of((16, TILE)))
        weight_y, slope_y = two_weights(index_y, frac[1], rows_of((16, TILE)))
        top_z, step_z = two_weights(index_z, frac[0], 16)
        top_y, step_y = two_weights(index_y, frac[1], 16)

        def over(block, weight):
            return jnp.sum(block * weight, axis=0, keepdims=True)

        on_z, on_y, on_edge = value[:16], value[16:32], value[32:33]
        dif_z, dif_y, dif_edge = diff[:16], diff[16:32], diff[32:33]
        grad_z = step_z * (over(on_z, weight_y) + top_y * on_edge) + top_y * over(on_y, slope_z)
        grad_y = top_z * (over(on_z, slope_y) + step_y * on_edge) + step_y * over(on_y, weight_z)
        grad_x = top_z * (over(dif_z, weight_y) + top_y * dif_edge) + top_y * over(dif_y, weight_z)
        grad_z = grad_z + grad_ref[0:1, lanes]
        grad_y = grad_y + grad_ref[1:2, lanes]
        grad_x = grad_x + grad_ref[2:3, lanes]
        slot = slots_ref[:, lanes].astype(F32)
        kind = rows_of((8, TILE)) & 3
        four = jnp.where(
            kind == 0, grad_z, jnp.where(kind == 1, grad_y, jnp.where(kind == 2, grad_x, slot))
        )
        owners = owners_ref[:, lanes]
        here = (rows_of((128, TILE)) >> 2) == (owners >> 6) * 2 + (owners & 1)
        for half, piece in enumerate(split(four)):
            tall = jnp.concatenate([piece.astype(F32)] * 16, 0)
            value_ref[half * 128 : (half + 1) * 128, lanes] = jnp.where(here, tall, 0.0).astype(BF16)
    both = lax.dot_general(
        value_ref[...], hot_ref[...], (((1,), (1,)), ((), ())), preferred_element_type=F32
    )
    send_ref[...] = both[:128] + both[128:]


def turn_kernel(in_ref, out_ref):
    out_ref[...] = in_ref[...].T


def place_kernel(recv_ref, out_ref, value_ref, hot_ref):
    turned = recv_ref[...].T
    high, low = split(turned)
    halves = (high.astype(F32), low.astype(F32))
    for j in range(32):
        lanes = slice(j * 128, (j + 1) * 128)
        slot = turned[4 * j + 3 : 4 * j + 4].astype(jnp.int32)
        here = (rows_of((64, 128)) >> 2) == (slot >> 7)
        for half, piece in enumerate(halves):
            four = piece[4 * j : 4 * j + 4]
            eight = jnp.concatenate([four, four], 0)
            tall = jnp.concatenate([eight] * 8, 0)
            value_ref[half * 64 : (half + 1) * 64, lanes] = jnp.where(here, tall, 0.0).astype(BF16)
        hot_ref[:, lanes] = hot_rows((128, 128), slot & 127)
    both = lax.dot_general(
        value_ref[...], hot_ref[...], (((1,), (1,)), ((), ())), preferred_element_type=F32
    )
    total = both[:64] + both[64:]
    for h in range(16):
        out_ref[:, h * 128 : (h + 1) * 128] = total[4 * h : 4 * h + 3]


def run_edge(face_z):
    return pl.pallas_call(
        edge_kernel,
        out_shape=jax.ShapeDtypeStruct((1, face_z.shape[1]), F32),
        compiler_params=SMALL,
        name="edge",
    )(face_z)


def run_face_y(plane, block_z):
    return pl.pallas_call(
        face_y_kernel,
        out_shape=jax.ShapeDtypeStruct((block_z, plane.shape[1]), F32),
        compiler_params=SMALL,
        name="face_y",
    )(plane)


def run_inner(plane, cells, offsets, owner_row):
    rows, size_x = plane.shape
    num_rows = cells.shape[1]
    return pl.pallas_call(
        inner_kernel,
        out_shape=(
            jax.ShapeDtypeStruct((8, num_rows), F32),
            jax.ShapeDtypeStruct((128, num_rows), BF16),
        ),
        scratch_shapes=[pltpu.VMEM((2 * rows, 2 * size_x), BF16)],
        compiler_params=SMALL,
        cost_estimate=pl.CostEstimate(
            flops=8 * rows * size_x * num_rows, bytes_accessed=1000000, transcendentals=0
        ),
        name="inner",
    )(plane, cells, offsets, owner_row)


def run_send(face_z, face_y, edge, grad, place, cells, offsets, owner_row, slot_row):
    num_rows = cells.shape[1]
    return pl.pallas_call(
        send_kernel,
        out_shape=jax.ShapeDtypeStruct((128, 128), F32),
        scratch_shapes=[
            pltpu.VMEM((160, edge.shape[1]), BF16),
            pltpu.VMEM((256, num_rows), BF16),
        ],
        compiler_params=SMALL,
        name="send",
    )(face_z, face_y, edge, grad, place, cells, offsets, owner_row, slot_row)


def run_turn(x):
    return pl.pallas_call(
        turn_kernel,
        out_shape=jax.ShapeDtypeStruct((128, 128), F32),
        compiler_params=SMALL,
        name="turn",
    )(x)


def run_place(received, num_rows):
    return pl.pallas_call(
        place_kernel,
        out_shape=jax.ShapeDtypeStruct((3, num_rows), F32),
        scratch_shapes=[pltpu.VMEM((128, 4096), BF16), pltpu.VMEM((128, 4096), BF16)],
        compiler_params=SMALL,
        name="place",
    )(received)


def body(grid_grad, cells, offsets, owners, slots):
    block_z, block_y, size_x = grid_grad.shape
    num_rows = cells.shape[1]
    count_z = lax.axis_size("gz")
    count_y = lax.axis_size("z") * lax.axis_size("c")
    next_z = [((i + 1) % count_z, i) for i in range(count_z)]
    next_y = [((i + 1) % count_y, i) for i in range(count_y)]
    next_zy = [
        (sz * count_y + sy, dz * count_y + dy) for sz, dz in next_z for sy, dy in next_y
    ]
    plane = grid_grad.reshape(block_z * block_y, size_x)
    face_z = grid_grad[0]
    edge = run_edge(face_z)
    face_y = run_face_y(plane, block_z)
    face_z = lax.ppermute(face_z, "gz", next_z)
    face_y = lax.ppermute(face_y, ("z", "c"), next_y)
    edge = lax.ppermute(edge, ("gz", "z", "c"), next_zy)
    owner_row = owners.reshape(1, num_rows)
    slot_row = slots.reshape(1, num_rows)
    grad, place = run_inner(plane, cells, offsets, owner_row)
    send = run_send(face_z, face_y, edge, grad, place, cells, offsets, owner_row, slot_row)
    in_plane = lax.all_to_all(send, ("gz", "c"), 0, 0, tiled=True)
    received = lax.all_to_all(run_turn(in_plane), "z", 0, 0, tiled=True)
    return run_place(received, num_rows)


def solution(mesh):
    fine = Mesh(mesh.devices.reshape(16, 32, 2), ("gz", "z", "c"))
    every = ("gz", "z", "c")
    placed = (P("gz", ("z", "c"), None), P(None, every), P(None, every), P(every, None), P(every))
    return jax.shard_map(
        body, mesh=fine, in_specs=placed, out_specs=P(None, every), check_vma=False
    )
```
